32 devices in a mesh: dp: 8 (over y, x, core), mp: 4 (over z).
Axes of the slice: x: 2, y: 2, z: 4, core: 2. Of those that a mesh axis runs over, the one named last changes fastest.
Arguments:
- tokens: bfloat16 [4096, 1024], P('dp', 'mp'), may hold values from -150 to 150
- pre_gain: bfloat16 [1024], P('mp'), may hold values from 0.25 to 1.75
- input_weight: bfloat16 [3, 1024, 1024], P(None, 'dp', 'mp'), may hold values from -0.125 to 0.125
- output_weight: bfloat16 [1024, 1024], P('mp', 'dp'), may hold values from -1 to 1
- position_bias: bfloat16 [16, 512, 512], P('mp'), may hold values from -3 to 353
- post_gain: bfloat16 [1024], P('mp'), may hold values from 0.25 to 1.75
Outputs:
- stream: bfloat16 [4096, 1024], P('dp', 'mp')
- normed: bfloat16 [4096, 1024], P('dp', 'mp')
The draws below stay inside these ranges and needn't reach their ends.
All inputs are finite; a program needn't handle non-finite values.
Results may differ from the reference program's by a relative error of at most 0.013.
Values may be sent and summed in bfloat16 or wider, within the bound.
A program may use at most 64 MiB of HBM per device.

```python
import math
import jax
import jax.numpy as jnp
from jax import lax

SEQ = 512
HEAD_DIM = 64
HEADS = 16
D = 1024
INNER = 1024
TOKENS = 4096


def draw_tokens(key, part):
    subkeys = jax.random.split(jax.random.fold_in(key, 11), 4)
    column_place = jnp.arange(D, dtype=jnp.float32) / D
    baseline = jnp.clip(jax.random.normal(subkeys[0], (TOKENS, D), jnp.float32), -4.0, 4.0)
    row_scale = jnp.exp(jax.random.uniform(subkeys[2], (TOKENS, 1), jnp.float32, math.log(0.4), math.log(4.0)))
    column_scale = jnp.exp(column_place * math.log(3.0))[None, :] * jnp.exp(jax.random.uniform(subkeys[3], (1, D), jnp.float32, math.log(0.7), math.log(1.4)))
    return (baseline * row_scale * column_scale).astype(jnp.bfloat16)


def draw_position_bias(key, part):
    subkeys = jax.random.split(jax.random.fold_in(key, 23), 1)
    bias_shape = (HEADS, SEQ, SEQ)
    return jnp.clip(jax.random.normal(subkeys[0], bias_shape, jnp.float32), -3.0, 3.0).astype(jnp.bfloat16)


def raised(drawn, stream_key, source, target, blocks, factor):
    owner, partner = [(jnp.arange(drawn.shape[axis_at]) // (drawn.shape[axis_at] // blocks)).reshape([-1 if axis == axis_at else 1 for axis in range(drawn.ndim)]) for axis_at in (source, target)]
    chosen = jax.random.permutation(stream_key, blocks)[partner]
    strong = (owner == chosen) | (owner == (partner + blocks // 2) % blocks)
    return jnp.where(strong, factor * drawn, drawn)


def block_levels(rng, dims, cuts, smallest, top_value):
    factor_of, own = 1.0, jax.random.fold_in(rng, 6)
    for dim, shards_of in cuts:
        steps = jnp.exp(jax.random.uniform(jax.random.fold_in(own, dim), (shards_of,), jnp.float32, smallest / len(cuts), top_value / len(cuts)))
        factor_of = factor_of * jnp.repeat(steps, dims[dim] // shards_of).reshape([-1 if axis == dim else 1 for axis in range(len(dims))])
    return factor_of


def normal_values(key, shape, width, reach, cuts=(), kind=jnp.bfloat16):
    entries = jax.random.normal(key, shape, jnp.float32) * width
    if len(cuts) > 0:
        entries = block_levels(key, shape, cuts, -0.22, 0.18) * entries
    return jnp.clip(entries, min=-reach, max=reach).astype(kind)


def heavy_noise(stream_key, shape, width, bound, cuts, heavy, kind=jnp.bfloat16):
    array = width * jax.random.normal(stream_key, shape, jnp.float32)
    if cuts:
        array = array * block_levels(stream_key, shape, cuts, -0.22, 0.18)
    return jnp.clip(raised(array, jax.random.fold_in(stream_key, 3), *heavy), -bound, bound).astype(kind)


def setup_inputs(seed: int = 0) -> dict:
    streams_of = jax.random.split(jax.random.key(seed), 7)
    return {
        "tokens": draw_tokens(jax.random.fold_in(streams_of[6], 71), 0),
        "pre_gain": jnp.clip(1.0 + 0.15 * jax.random.normal(streams_of[1], (D,), jnp.float32), 0.25, 1.75).astype(jnp.bfloat16),
        "input_weight": normal_values(streams_of[2], (3, D, INNER), (2 * D) ** -0.5, 0.125, ((1, 8), (2, 4))),
        "output_weight": heavy_noise(streams_of[3], (INNER, D), (INNER // 16) ** -0.5, 1.0, ((0, 4), (1, 8)), (0, 1, 8, 2.0)),
        "position_bias": draw_position_bias(jax.random.fold_in(streams_of[6], 71), 0),
        "post_gain": jnp.clip(1.0 + 0.15 * jax.random.normal(streams_of[5], (D,), jnp.float32), 0.25, 1.75).astype(jnp.bfloat16),
    }


epsilon = 1e-06

def reference(tokens, pre_gain, input_weight, output_weight, position_bias, post_gain):
    widened = tokens.astype(jnp.float32)
    inverse_rms = lax.rsqrt(lax.optimization_barrier(jnp.mean(widened * widened, axis=1, keepdims=True)) + epsilon)
    normed_in = (widened * inverse_rms * pre_gain.astype(jnp.float32)).astype(jnp.bfloat16)
    projected = [jnp.dot(normed_in, input_weight[member], preferred_element_type=jnp.float32).astype(jnp.bfloat16) for member in range(3)]
    row_count = tokens.shape[0]
    bias_wide = position_bias.astype(jnp.float32)

    def one_sequence(sequence):
        offset = (sequence * SEQ).astype(jnp.int32)
        sliced = [lax.dynamic_slice_in_dim(matrix, offset, SEQ, 0).reshape(SEQ, HEADS, HEAD_DIM).astype(jnp.float32) for matrix in projected]
        scores = jnp.einsum('qhd,khd->hqk', sliced[0], sliced[1]) + bias_wide
        row_max = lax.optimization_barrier(jnp.max(scores, axis=2, keepdims=True))
        weights = jnp.exp(scores - row_max)
        probabilities = (weights / lax.optimization_barrier(jnp.sum(weights, axis=2, keepdims=True))).astype(jnp.bfloat16)
        context = jnp.einsum('hqk,khd->qhd', probabilities.astype(jnp.float32), sliced[2])
        return context.reshape(SEQ, HEADS * HEAD_DIM).astype(jnp.bfloat16)
    stacked = lax.map(one_sequence, jnp.arange(row_count // SEQ, dtype=jnp.int32))
    context = stacked.reshape(row_count, HEADS * HEAD_DIM)
    attention_out = jnp.dot(context, output_weight, preferred_element_type=jnp.float32)
    stream = (widened + attention_out).astype(jnp.bfloat16)
    restored = lax.optimization_barrier(stream).astype(jnp.float32)
    post_rms = lax.rsqrt(lax.optimization_barrier(jnp.mean(restored * restored, axis=1, keepdims=True)) + epsilon)
    normed = (restored * post_rms * post_gain.astype(jnp.float32)).astype(jnp.bfloat16)
    return (stream, normed)
```

```python
import functools

import jax
import jax.numpy as jnp
from jax import lax
from jax.experimental import pallas as pl
from jax.experimental.pallas import tpu as pltpu
from jax.sharding import PartitionSpec as P

epsilon = 1e-06
F32, BF16 = jnp.float32, jnp.bfloat16


def kernel(
    n,
    groups,
    chunks,
    wide,
    tok,
    gains,
    win,
    wout,
    bias,
    stream_o,
    normed_o,
    x_all,
    gain_all,
    w_all,
    wo_all,
    bias_v,
    acc,
    square,
    qkv,
    part,
    out_buf,
    from_below,
    from_above,
    ss_mine,
    ss_all,
    ag_send,
    ag_recv,
    g_send,
    g_recv,
    w_send,
    w_recv,
    o_send,
    o_recv,
    rs_send,
    rs_recv,
    ss_send,
    ss_recv,
    local_sem,
):
    rows, feats = tok.shape
    step = rows // chunks
    heads, seq = bias.shape[0], bias.shape[1]
    inner = win.shape[2]
    head_dim = inner // heads
    model = n * feats
    wrows = win.shape[1]
    wcols = model // groups
    half = groups // 2
    me = lax.axis_index("mp")
    d = lax.axis_index("dp")
    odd = lax.rem(d, 2)
    pair = d // 2
    partner = d + 1 - 2 * odd

    def rows_at(c):
        return pl.ds(pl.multiple_of(c * step, step), step)

    def tok_copy(s, c, up, own):
        src = tok.at[rows_at(c)] if own else x_all.at[s, rows_at(c)]
        return pltpu.make_async_remote_copy(
            src_ref=src,
            dst_ref=x_all.at[s, rows_at(c)],
            send_sem=ag_send.at[up, s, c],
            recv_sem=ag_recv.at[s, c],
            device_id={"mp": me + 2 * up - 1},
            device_id_type=pl.DeviceIdType.MESH,
        )

    def gain_copy(origin, target):
        return pltpu.make_async_remote_copy(
            src_ref=gains,
            dst_ref=gain_all.at[origin],
            send_sem=g_send.at[target],
            recv_sem=g_recv.at[origin],
            device_id={"mp": target},
            device_id_type=pl.DeviceIdType.MESH,
        )

    def w_slot(o):
        return w_all.at[:, pl.ds(pl.multiple_of(o * wrows, wrows), wrows), :]

    def o_slot(o):
        block = pl.ds(pl.multiple_of(o * wcols, wcols), wcols)
        return wo_all.at[:, block] if wide else wo_all.at[block, :]

    def weight_copy(which, o, target, forward):
        slot, ref, send, recv = (
            (w_slot, win, w_send, w_recv) if which == 0 else (o_slot, wout, o_send, o_recv)
        )
        return pltpu.make_async_remote_copy(
            src_ref=slot(o) if forward else ref,
            dst_ref=slot(o),
            send_sem=send.at[1, o] if forward else send.at[0, target],
            recv_sem=recv.at[o],
            device_id={"dp": target},
            device_id_type=pl.DeviceIdType.MESH,
        )

    def rs_copy(s, c, up):
        return pltpu.make_async_remote_copy(
            src_ref=out_buf.at[s, rows_at(c)],
            dst_ref=(from_below if up else from_above).at[s, rows_at(c)],
            send_sem=rs_send.at[s, c],
            recv_sem=rs_recv.at[up, s, c],
            device_id={"mp": me + 2 * up - 1},
            device_id_type=pl.DeviceIdType.MESH,
        )

    def ss_copy(origin, c, target):
        return pltpu.make_async_remote_copy(
            src_ref=ss_mine.at[c],
            dst_ref=ss_all.at[origin, c],
            send_sem=ss_send.at[target, c],
            recv_sem=ss_recv.at[origin, c],
            device_id={"mp": target},
            device_id_type=pl.DeviceIdType.MESH,
        )

    def loop(count, body, start=0):
        def wrapped(i, carry):
            body(i)
            return carry

        lax.fori_loop(start, count, wrapped, 0)

    def local_copies():
        return (
            pltpu.make_async_copy(win, w_slot(d), local_sem.at[0]),
            pltpu.make_async_copy(wout, o_slot(d), local_sem.at[1]),
            pltpu.make_async_copy(tok, x_all.at[me], local_sem.at[2]),
            pltpu.make_async_copy(gains, gain_all.at[me], local_sem.at[3]),
            pltpu.make_async_copy(bias, bias_v, local_sem.at[4]),
        )

    for copy in local_copies():
        copy.start()

    barrier = pltpu.get_barrier_semaphore()

    def greet_mp(k):
        pl.semaphore_signal(
            barrier,
            inc=1,
            device_id={"mp": lax.rem(me + k, n)},
            device_id_type=pl.DeviceIdType.MESH,
        )

    def greet_dp(k):
        pl.semaphore_signal(
            barrier,
            inc=1,
            device_id={"dp": lax.rem(d + k, groups)},
            device_id_type=pl.DeviceIdType.MESH,
        )

    loop(n, greet_mp, 1)
    loop(groups, greet_dp, 1)
    pl.semaphore_wait(barrier, n - 1 + groups - 1)

    def peer_mp(k):
        return lax.rem(me + k, n)

    def same_core(k):
        return 2 * lax.rem(pair + k, half) + odd

    def from_core(k):
        return 2 * lax.rem(pair + half - k, half) + odd

    loop(n, lambda k: gain_copy(me, peer_mp(k)).start(), 1)
    for c in range(chunks):

        @pl.when(me < n - 1)
        def _():
            tok_copy(me, c, 1, True).start()

        @pl.when(me > 0)
        def _():
            tok_copy(me, c, 0, True).start()

    weight_copy(0, d, partner, False).start()
    loop(half, lambda k: weight_copy(0, d, same_core(k), False).start(), 1)
    weight_copy(1, d, partner, False).start()
    loop(half, lambda k: weight_copy(1, d, same_core(k), False).start(), 1)

    acc[...] = jnp.zeros_like(acc)
    square[...] = jnp.zeros_like(square)

    def take_shards(j):
        below, above = me - j, me + j

        def one(c):
            @pl.when(below >= 0)
            def _():
                tok_copy(below, c, 1, False).wait_recv()

                @pl.when(me < n - 1)
                def _():
                    tok_copy(below, c, 1, False).start()

            @pl.when(above < n)
            def _():
                tok_copy(above, c, 0, False).wait_recv()

                @pl.when(me > 0)
                def _():
                    tok_copy(above, c, 0, False).start()

        loop(chunks, one)

    def project(j):
        def side(up):
            s = me + (2 * up - 1) * j

            @pl.when((s >= 0) & (s < n) & ((j > 0) | (up == 0)))
            def _():
                block = pl.ds(pl.multiple_of(s * feats, feats), feats)
                gain = gain_all[s][0:1, :]

                def piece(c):
                    x = x_all[s, rows_at(c), :].astype(F32)
                    square[rows_at(c), :] += x * x
                    xg = (x * gain).astype(BF16)
                    for m in range(3):
                        acc[m, rows_at(c), :] += jnp.dot(
                            xg, w_all[m, block, :], preferred_element_type=F32
                        )

                loop(chunks, piece)

        loop(2, side)

    def weights_in(which):
        def forward(k):
            o = from_core(k)
            weight_copy(which, o, partner, False).wait_recv()
            weight_copy(which, o, partner, True).start()

        loop(half, forward, 1)

        def others(k):
            weight_copy(which, 2 * k + 1 - odd, partner, False).wait_recv()

        loop(half, others)

    take_shards(1)
    for copy in local_copies():
        copy.wait()
    loop(n, lambda k: gain_copy(peer_mp(k), peer_mp(k)).wait_recv(), 1)
    weights_in(0)
    loop(2, project)

    def later(j):
        take_shards(j)
        project(j)

    loop(n, later, 2)
    weights_in(1)

    def finish(c):
        total = jnp.sum(square[rows_at(c), :], axis=1, keepdims=True)
        inverse = lax.rsqrt(total / model + epsilon)
        for m in range(3):
            qkv[m, rows_at(c), :] = (acc[m, rows_at(c), :] * inverse).astype(BF16)

    loop(chunks, finish)

    lane_head = lax.broadcasted_iota(jnp.int32, (1, inner), 1) // head_dim
    contract = (((1,), (1,)), ((), ()))

    def send_out(s, c, up, value):
        out_buf[s, rows_at(c), :] = value.astype(BF16)
        rs_copy(s, c, up).start()

    def attend(c):
        first = (c * step) // seq * seq
        keys_at = pl.ds(pl.multiple_of(first, seq), seq)
        bias_at = pl.ds(pl.multiple_of(c * step - first, step), step)
        q = qkv[0, rows_at(c), :]
        k = qkv[1, keys_at, :]
        v = qkv[2, keys_at, :]
        context = jnp.zeros((step, inner), F32)
        for h in range(heads):
            qh = jnp.where(lane_head == h, q, jnp.zeros_like(q))
            scores = lax.dot_general(qh, k, contract, preferred_element_type=F32)
            scores = scores + bias_v[h, bias_at, :].astype(F32)
            weights = jnp.exp(scores - jnp.max(scores, axis=1, keepdims=True))
            scale = 1.0 / jnp.sum(weights, axis=1, keepdims=True)
            mixed = jnp.dot(weights.astype(BF16), v, preferred_element_type=F32)
            context = jnp.where(lane_head == h, mixed * scale, context)
        context = context.astype(BF16)

        def share(s):
            block = pl.ds(pl.multiple_of(s * feats, feats), feats)
            if wide:
                value = jnp.dot(context, wo_all[:, block], preferred_element_type=F32)
            else:
                value = lax.dot_general(
                    context, wo_all[block, :], contract, preferred_element_type=F32
                )
            part[s, rows_at(c), :] = value

        for s in range(n):
            share(s)

        @pl.when(me == 0)
        def _():
            loop(n - 1, lambda k: send_out(n - 1 - k, c, 1, part[n - 1 - k, rows_at(c), :]))

        @pl.when(me == n - 1)
        def _():
            loop(n - 1, lambda k: send_out(k, c, 0, part[k, rows_at(c), :]))

    loop(rows // step, attend)

    def reduce(c):
        def hop(k):
            up_s, down_s = n - 1 - k, k

            @pl.when((up_s > me) & (me > 0))
            def _():
                rs_copy(up_s, c, 1).wait_recv()
                send_out(
                    up_s,
                    c,
                    1,
                    part[up_s, rows_at(c), :] + from_below[up_s, rows_at(c), :].astype(F32),
                )

            @pl.when((down_s < me) & (me < n - 1))
            def _():
                rs_copy(down_s, c, 0).wait_recv()
                send_out(
                    down_s,
                    c,
                    0,
                    part[down_s, rows_at(c), :] + from_above[down_s, rows_at(c), :].astype(F32),
                )

        loop(n - 1, hop)

        @pl.when(me > 0)
        def _():
            rs_copy(me, c, 1).wait_recv()
            part[me, rows_at(c), :] += from_below[me, rows_at(c), :].astype(F32)

        @pl.when(me < n - 1)
        def _():
            rs_copy(me, c, 0).wait_recv()
            part[me, rows_at(c), :] += from_above[me, rows_at(c), :].astype(F32)

        stream = (x_all[me, rows_at(c), :].astype(F32) + part[me, rows_at(c), :]).astype(BF16)
        stream_o[rows_at(c), :] = stream
        wide_stream = stream.astype(F32)
        total = jnp.sum(wide_stream * wide_stream, axis=1, keepdims=True)
        turned = jnp.transpose(jnp.broadcast_to(total, (step, 128)))
        ss_mine[c] = turned[0:8, :]
        ss_all[me, c] = turned[0:8, :]
        loop(n, lambda k: ss_copy(me, c, peer_mp(k)).start(), 1)

    loop(chunks, reduce)

    def normalize(c):
        loop(n, lambda k: ss_copy(peer_mp(k), c, peer_mp(k)).wait_recv(), 1)
        total = jnp.zeros((8, step), F32)
        for s in range(n):
            total = total + ss_all[s, c]
        post = jnp.transpose(lax.rsqrt(total / model + epsilon))[:, 0:1]
        stream = stream_o[rows_at(c), :].astype(F32)
        gain = gain_all[me][1:2, :]
        normed_o[rows_at(c), :] = (stream * post * gain).astype(BF16)

    loop(chunks, normalize)

    loop(n, lambda k: gain_copy(me, peer_mp(k)).wait_send(), 1)

    def drain_tokens(s):
        def one(c):
            @pl.when((s <= me) & (me < n - 1))
            def _():
                tok_copy(s, c, 1, False).wait_send()

            @pl.when((s >= me) & (me > 0))
            def _():
                tok_copy(s, c, 0, False).wait_send()

            @pl.when(s != me)
            def _():
                rs_copy(s, c, 1).wait_send()
                ss_copy(me, c, s).wait_send()

        loop(chunks, one)

    loop(n, drain_tokens)
    for which in range(2):
        weight_copy(which, d, partner, False).wait_send()

        def drain(k):
            weight_copy(which, d, same_core(k), False).wait_send()
            weight_copy(which, from_core(k), partner, True).wait_send()

        loop(half, drain, 1)


def on_device(n, groups, tokens, pre_gain, input_weight, output_weight, position_bias, post_gain):
    rows, feats = tokens.shape
    chunks = rows // 128
    step = rows // chunks
    inner = input_weight.shape[2]
    model = n * feats
    wide = output_weight.shape[1] % 128 == 0
    gains = jnp.stack([pre_gain, post_gain]).astype(F32)
    if not wide:
        output_weight = output_weight.T
    dma, any_space = pltpu.SemaphoreType.DMA, pl.BlockSpec(memory_space=pl.ANY)
    shape = jax.ShapeDtypeStruct((rows, feats), BF16)
    return pl.pallas_call(
        functools.partial(kernel, n, groups, chunks, wide),
        out_shape=(shape, shape),
        in_specs=[any_space] * 5,
        out_specs=[pl.BlockSpec(memory_space=pltpu.VMEM)] * 2,
        scratch_shapes=[
            pltpu.VMEM((n, rows, feats), BF16),
            pltpu.VMEM((n, 2, feats), F32),
            pltpu.VMEM((3, model, inner), BF16),
            pltpu.VMEM((inner, model) if wide else (model, inner), BF16),
            pltpu.VMEM(position_bias.shape, BF16),
            pltpu.VMEM((3, rows, inner), F32),
            pltpu.VMEM((rows, feats), F32),
            pltpu.VMEM((3, rows, inner), BF16),
            pltpu.VMEM((n, rows, feats), F32),
            pltpu.VMEM((n, rows, feats), BF16),
            pltpu.VMEM((n, rows, feats), BF16),
            pltpu.VMEM((n, rows, feats), BF16),
            pltpu.VMEM((chunks, 8, step), F32),
            pltpu.VMEM((n, chunks, 8, step), F32),
            dma((2, n, chunks)),
            dma((n, chunks)),
            dma((n,)),
            dma((n,)),
            dma((2, groups)),
            dma((groups,)),
            dma((2, groups)),
            dma((groups,)),
            dma((n, chunks)),
            dma((2, n, chunks)),
            dma((n, chunks)),
            dma((n, chunks)),
            dma((5,)),
        ],
        compiler_params=pltpu.CompilerParams(
            collective_id=0, has_side_effects=True, vmem_limit_bytes=56 * 1024 * 1024
        ),
    )(tokens, gains, input_weight, output_weight, position_bias)


def solution(mesh):
    return jax.shard_map(
        functools.partial(on_device, mesh.shape["mp"], mesh.shape["dp"]),
        mesh=mesh,
        in_specs=(
            P("dp", "mp"),
            P("mp"),
            P(None, "dp", "mp"),
            P("mp", "dp"),
            P("mp", None, None),
            P("mp"),
        ),
        out_specs=(P("dp", "mp"), P("dp", "mp")),
        check_vma=False,
    )
```

```python
import functools

import jax
import jax.numpy as jnp
from jax import lax
from jax.experimental import pallas as pl
from jax.experimental.pallas import tpu as pltpu
from jax.sharding import PartitionSpec as P

epsilon = 1e-06
F32, BF16 = jnp.float32, jnp.bfloat16


def kernel(
    n,
    groups,
    chunks,
    lag,
    wide,
    tok,
    pre,
    post_g,
    win,
    wout,
    bias,
    stream_o,
    normed_o,
    x_all,
    gain_all,
    w_all,
    wo_all,
    bias_v,
    acc,
    square,
    qkv,
    part,
    out_buf,
    from_below,
    from_above,
    ss_mine,
    ss_all,
    ag_send,
    ag_recv,
    g_send,
    g_recv,
    w_send,
    w_recv,
    o_send,
    o_recv,
    rs_send,
    rs_recv,
    ss_send,
    ss_recv,
    local_sem,
):
    rows, feats = tok.shape
    step = rows // chunks
    heads, seq = bias.shape[0], bias.shape[1]
    inner = win.shape[2]
    head_dim = inner // heads
    model = n * feats
    wrows = win.shape[1]
    wcols = model // groups
    half = groups // 2
    me = lax.axis_index("mp")
    d = lax.axis_index("dp")
    odd = lax.rem(d, 2)
    pair = d // 2
    partner = d + 1 - 2 * odd

    def rows_at(c):
        return pl.ds(pl.multiple_of(c * step, step), step)

    def feats_at(s):
        return pl.ds(pl.multiple_of(s * feats, feats), feats)

    def tok_copy(s, c, up, own):
        src = tok.at[rows_at(c)] if own else x_all.at[s, rows_at(c)]
        return pltpu.make_async_remote_copy(
            src_ref=src,
            dst_ref=x_all.at[s, rows_at(c)],
            send_sem=ag_send.at[up, s, c],
            recv_sem=ag_recv.at[s, c],
            device_id={"mp": me + 2 * up - 1},
            device_id_type=pl.DeviceIdType.MESH,
        )

    def gain_copy(origin, target):
        return pltpu.make_async_remote_copy(
            src_ref=pre,
            dst_ref=gain_all.at[feats_at(origin)],
            send_sem=g_send.at[target],
            recv_sem=g_recv.at[origin],
            device_id={"mp": target},
            device_id_type=pl.DeviceIdType.MESH,
        )

    def w_slot(o):
        return w_all.at[:, pl.ds(pl.multiple_of(o * wrows, wrows), wrows), :]

    def o_slot(o):
        block = pl.ds(pl.multiple_of(o * wcols, wcols), wcols)
        return wo_all.at[:, block] if wide else wo_all.at[block, :]

    def weight_copy(which, o, target, forward):
        slot, ref, send, recv = (
            (w_slot, win, w_send, w_recv) if which == 0 else (o_slot, wout, o_send, o_recv)
        )
        return pltpu.make_async_remote_copy(
            src_ref=slot(o) if forward else ref,
            dst_ref=slot(o),
            send_sem=send.at[1, o] if forward else send.at[0, target],
            recv_sem=recv.at[o],
            device_id={"dp": target},
            device_id_type=pl.DeviceIdType.MESH,
        )

    def rs_copy(s, c, up):
        return pltpu.make_async_remote_copy(
            src_ref=out_buf.at[s, rows_at(c)],
            dst_ref=(from_below if up else from_above).at[s, rows_at(c)],
            send_sem=rs_send.at[s, c],
            recv_sem=rs_recv.at[up, s, c],
            device_id={"mp": me + 2 * up - 1},
            device_id_type=pl.DeviceIdType.MESH,
        )

    def ss_copy(origin, c, target):
        return pltpu.make_async_remote_copy(
            src_ref=ss_mine.at[c],
            dst_ref=ss_all.at[origin, c],
            send_sem=ss_send.at[target, c],
            recv_sem=ss_recv.at[origin, c],
            device_id={"mp": target},
            device_id_type=pl.DeviceIdType.MESH,
        )

    def loop(count, body, start=0):
        def wrapped(i, carry):
            body(i)
            return carry

        lax.fori_loop(start, count, wrapped, 0)

    def local_copies():
        return (
            pltpu.make_async_copy(win, w_slot(d), local_sem.at[0]),
            pltpu.make_async_copy(wout, o_slot(d), local_sem.at[1]),
            pltpu.make_async_copy(tok, x_all.at[me], local_sem.at[2]),
            pltpu.make_async_copy(pre, gain_all.at[feats_at(me)], local_sem.at[3]),
            pltpu.make_async_copy(bias, bias_v, local_sem.at[4]),
        )

    for copy in local_copies():
        copy.start()

    barrier = pltpu.get_barrier_semaphore()

    def greet_mp(k):
        pl.semaphore_signal(
            barrier,
            inc=1,
            device_id={"mp": lax.rem(me + k, n)},
            device_id_type=pl.DeviceIdType.MESH,
        )

    def greet_dp(k):
        pl.semaphore_signal(
            barrier,
            inc=1,
            device_id={"dp": lax.rem(d + k, groups)},
            device_id_type=pl.DeviceIdType.MESH,
        )

    loop(n, greet_mp, 1)
    loop(groups, greet_dp, 1)
    pl.semaphore_wait(barrier, n - 1 + groups - 1)

    def peer_mp(k):
        return lax.rem(me + k, n)

    def same_core(k):
        return 2 * lax.rem(pair + k, half) + odd

    def from_core(k):
        return 2 * lax.rem(pair + half - k, half) + odd

    loop(n, lambda k: gain_copy(me, peer_mp(k)).start(), 1)
    for c in range(chunks):

        @pl.when(me < n - 1)
        def _():
            tok_copy(me, c, 1, True).start()

        @pl.when(me > 0)
        def _():
            tok_copy(me, c, 0, True).start()

    weight_copy(0, d, partner, False).start()
    loop(half, lambda k: weight_copy(0, d, same_core(k), False).start(), 1)
    weight_copy(1, d, partner, False).start()
    loop(half, lambda k: weight_copy(1, d, same_core(k), False).start(), 1)

    acc[...] = jnp.zeros_like(acc)
    square[...] = jnp.zeros_like(square)

    def take_shards(j):
        below, above = me - j, me + j

        def one(c):
            @pl.when(below >= 0)
            def _():
                tok_copy(below, c, 1, False).wait_recv()

                @pl.when(me < n - 1)
                def _():
                    tok_copy(below, c, 1, False).start()

            @pl.when(above < n)
            def _():
                tok_copy(above, c, 0, False).wait_recv()

                @pl.when(me > 0)
                def _():
                    tok_copy(above, c, 0, False).start()

        loop(chunks, one)

    def project(j):
        def side(up):
            s = me + (2 * up - 1) * j

            @pl.when((s >= 0) & (s < n) & ((j > 0) | (up == 0)))
            def _():
                block = feats_at(s)
                gain = gain_all[feats_at(s)].astype(F32).reshape(1, feats)

                x = x_all[s].astype(F32)
                square[...] += x * x
                xg = (x * gain).astype(BF16)
                for m in range(3):
                    acc[m] += jnp.dot(xg, w_all[m, block, :], preferred_element_type=F32)

        loop(2, side)

    def weights_in(which):
        def forward(k):
            o = from_core(k)
            weight_copy(which, o, partner, False).wait_recv()
            weight_copy(which, o, partner, True).start()

        loop(half, forward, 1)

        def others(k):
            weight_copy(which, 2 * k + 1 - odd, partner, False).wait_recv()

        loop(half, others)

    take_shards(1)
    for copy in local_copies():
        copy.wait()
    loop(n, lambda k: gain_copy(peer_mp(k), peer_mp(k)).wait_recv(), 1)
    weights_in(0)
    loop(2, project)

    def later(j):
        take_shards(j)
        project(j)

    loop(n, later, 2)
    weights_in(1)

    def finish(c):
        total = jnp.sum(square[rows_at(c), :], axis=1, keepdims=True)
        inverse = lax.rsqrt(total / model + epsilon)
        for m in range(3):
            qkv[m, rows_at(c), :] = (acc[m, rows_at(c), :] * inverse).astype(BF16)

    loop(chunks, finish)

    lane_head = lax.broadcasted_iota(jnp.int32, (1, inner), 1) // head_dim
    contract = (((1,), (1,)), ((), ()))

    def send_out(s, c, up, value):
        out_buf[s, rows_at(c), :] = value.astype(BF16)
        rs_copy(s, c, up).start()

    def attend(c):
        first = (c * step) // seq * seq
        keys_at = pl.ds(pl.multiple_of(first, seq), seq)
        bias_at = pl.ds(pl.multiple_of(c * step - first, step), step)
        q = qkv[0, rows_at(c), :]
        k = qkv[1, keys_at, :]
        v = qkv[2, keys_at, :]
        context = jnp.zeros((step, inner), F32)
        for h in range(heads):
            qh = jnp.where(lane_head == h, q, jnp.zeros_like(q))
            scores = lax.dot_general(qh, k, contract, preferred_element_type=F32)
            scores = scores + bias_v[h, bias_at, :].astype(F32)
            weights = jnp.exp(scores - jnp.max(scores, axis=1, keepdims=True))
            scale = 1.0 / jnp.sum(weights, axis=1, keepdims=True)
            mixed = jnp.dot(weights.astype(BF16), v, preferred_element_type=F32)
            context = jnp.where(lane_head == h, mixed * scale, context)
        context = context.astype(BF16)

        def share(s):
            block = feats_at(s)
            if wide:
                value = jnp.dot(context, wo_all[:, block], preferred_element_type=F32)
            else:
                value = lax.dot_general(
                    context, wo_all[block, :], contract, preferred_element_type=F32
                )
            part[s, rows_at(c), :] = value

        for s in range(n):
            share(s)

        @pl.when(me == 0)
        def _():
            loop(n - 1, lambda k: send_out(n - 1 - k, c, 1, part[n - 1 - k, rows_at(c), :]))

        @pl.when(me == n - 1)
        def _():
            loop(n - 1, lambda k: send_out(k, c, 0, part[k, rows_at(c), :]))

    loop(rows // step, attend)

    def finalize(c):
        own = x_all[me, rows_at(c), :].astype(F32) + part[me, rows_at(c), :]
        stream = own.astype(BF16)
        stream_o[rows_at(c), :] = stream
        wide_stream = stream.astype(F32)
        total = jnp.sum(wide_stream * wide_stream, axis=1, keepdims=True)
        turned = jnp.transpose(jnp.broadcast_to(total, (step, 128)))
        ss_mine[c] = turned[0:8, :]
        ss_all[me, c] = turned[0:8, :]
        loop(n, lambda k: ss_copy(me, c, peer_mp(k)).start(), 1)

    messages = chunks * (n - 1)

    def chain(t, up, lead):
        m = t - lead
        landed = from_below if up else from_above

        @pl.when((m >= 0) & (m < messages))
        def _():
            c, k = m // (n - 1), lax.rem(m, n - 1)
            s = n - 1 - k if up else k
            further = s > me if up else s < me

            @pl.when(further | (s == me))
            def _():
                rs_copy(s, c, up).wait_recv()
                value = part[s, rows_at(c), :] + landed[s, rows_at(c), :].astype(F32)

                @pl.when(s == me)
                def _():
                    part[s, rows_at(c), :] = value

                @pl.when(further)
                def _():
                    send_out(s, c, up, value)

    up_lead, down_lead = (me - 1) * lag, (n - 2 - me) * lag
    up_last, down_last = n - 1 - me + up_lead, me + down_lead
    last = jnp.where(
        me == 0, down_last, jnp.where(me == n - 1, up_last, jnp.maximum(up_last, down_last))
    )

    def tick(t):
        @pl.when(me > 0)
        def _():
            chain(t, 1, up_lead)

        @pl.when(me < n - 1)
        def _():
            chain(t, 0, down_lead)

        @pl.when((t >= last) & (lax.rem(t - last + n - 1, n - 1) == 0))
        def _():
            c = (t - last + n - 1) // (n - 1) - 1

            @pl.when(c < chunks)
            def _():
                finalize(c)

    loop(messages + (n - 2) * lag, tick)

    def normalize(c):
        loop(n, lambda k: ss_copy(peer_mp(k), c, peer_mp(k)).wait_recv(), 1)
        total = jnp.zeros((8, step), F32)
        for s in range(n):
            total = total + ss_all[s, c]
        post = jnp.transpose(lax.rsqrt(total / model + epsilon))[:, 0:1]
        stream = stream_o[rows_at(c), :].astype(F32)
        gain = post_g[...].astype(F32).reshape(1, feats)
        normed_o[rows_at(c), :] = (stream * post * gain).astype(BF16)

    loop(chunks, normalize)

    loop(n, lambda k: gain_copy(me, peer_mp(k)).wait_send(), 1)

    def drain_tokens(s):
        def one(c):
            @pl.when((s <= me) & (me < n - 1))
            def _():
                tok_copy(s, c, 1, False).wait_send()

            @pl.when((s >= me) & (me > 0))
            def _():
                tok_copy(s, c, 0, False).wait_send()

            @pl.when(s != me)
            def _():
                rs_copy(s, c, 1).wait_send()
                ss_copy(me, c, s).wait_send()

        loop(chunks, one)

    loop(n, drain_tokens)
    for which in range(2):
        weight_copy(which, d, partner, False).wait_send()

        def drain(k):
            weight_copy(which, d, same_core(k), False).wait_send()
            weight_copy(which, from_core(k), partner, True).wait_send()

        loop(half, drain, 1)


def on_device(n, groups, tokens, pre_gain, input_weight, output_weight, position_bias, post_gain):
    rows, feats = tokens.shape
    chunks, lag = rows // 256, 2
    step = rows // chunks
    inner = input_weight.shape[2]
    model = n * feats
    wide = output_weight.shape[1] % 128 == 0
    if not wide:
        output_weight = output_weight.T
    dma, any_space = pltpu.SemaphoreType.DMA, pl.BlockSpec(memory_space=pl.ANY)
    shape = jax.ShapeDtypeStruct((rows, feats), BF16)
    return pl.pallas_call(
        functools.partial(kernel, n, groups, chunks, lag, wide),
        out_shape=(shape, shape),
        in_specs=[any_space] * 2 + [pl.BlockSpec(memory_space=pltpu.VMEM)] + [any_space] * 3,
        out_specs=[pl.BlockSpec(memory_space=pltpu.VMEM)] * 2,
        scratch_shapes=[
            pltpu.VMEM((n, rows, feats), BF16),
            pltpu.VMEM((n * feats,), BF16),
            pltpu.VMEM((3, model, inner), BF16),
            pltpu.VMEM((inner, model) if wide else (model, inner), BF16),
            pltpu.VMEM(position_bias.shape, BF16),
            pltpu.VMEM((3, rows, inner), F32),
            pltpu.VMEM((rows, feats), F32),
            pltpu.VMEM((3, rows, inner), BF16),
            pltpu.VMEM((n, rows, feats), F32),
            pltpu.VMEM((n, rows, feats), BF16),
            pltpu.VMEM((n, rows, feats), BF16),
            pltpu.VMEM((n, rows, feats), BF16),
            pltpu.VMEM((chunks, 8, step), F32),
            pltpu.VMEM((n, chunks, 8, step), F32),
            dma((2, n, chunks)),
            dma((n, chunks)),
            dma((n,)),
            dma((n,)),
            dma((2, groups)),
            dma((groups,)),
            dma((2, groups)),
            dma((groups,)),
            dma((n, chunks)),
            dma((2, n, chunks)),
            dma((n, chunks)),
            dma((n, chunks)),
            dma((5,)),
        ],
        compiler_params=pltpu.CompilerParams(
            collective_id=0, has_side_effects=True, vmem_limit_bytes=56 * 1024 * 1024
        ),
    )(tokens, pre_gain, post_gain, input_weight, output_weight, position_bias)


def solution(mesh):
    return jax.shard_map(
        functools.partial(on_device, mesh.shape["mp"], mesh.shape["dp"]),
        mesh=mesh,
        in_specs=(
            P("dp", "mp"),
            P("mp"),
            P(None, "dp", "mp"),
            P("mp", "dp"),
            P("mp", None, None),
            P("mp"),
        ),
        out_specs=(P("dp", "mp"), P("dp", "mp")),
        check_vma=False,
    )
```

```python
import functools

import jax
import jax.numpy as jnp
from jax import lax
from jax.experimental import pallas as pl
from jax.experimental.pallas import tpu as pltpu
from jax.sharding import PartitionSpec as P

epsilon = 1e-06
F32, BF16 = jnp.float32, jnp.bfloat16


def kernel(
    n,
    groups,
    chunks,
    lag,
    wide,
    tok,
    pre,
    post_g,
    win,
    wout,
    bias,
    stream_o,
    normed_o,
    x_all,
    gain_all,
    w_all,
    wo_all,
    bias_v,
    acc,
    square,
    qkv,
    part,
    out_buf,
    from_below,
    from_above,
    ss_mine,
    ss_all,
    ag_send,
    ag_recv,
    g_send,
    g_recv,
    w_send,
    w_recv,
    o_send,
    o_recv,
    rs_send,
    rs_recv,
    ss_send,
    ss_recv,
    local_sem,
    link_free,
):
    rows, feats = tok.shape
    step = rows // chunks
    heads, seq = bias.shape[0], bias.shape[1]
    inner = win.shape[2]
    head_dim = inner // heads
    model = n * feats
    wrows = win.shape[1]
    wcols = model // groups
    half = groups // 2
    me = lax.axis_index("mp")
    d = lax.axis_index("dp")
    odd = lax.rem(d, 2)
    pair = d // 2
    partner = d + 1 - 2 * odd

    def rows_at(c):
        return pl.ds(pl.multiple_of(c * step, step), step)

    def feats_at(s):
        return pl.ds(pl.multiple_of(s * feats, feats), feats)

    def tok_copy(s, c, up, own):
        src = tok.at[rows_at(c)] if own else x_all.at[s, rows_at(c)]
        return pltpu.make_async_remote_copy(
            src_ref=src,
            dst_ref=x_all.at[s, rows_at(c)],
            send_sem=ag_send.at[up, s, c],
            recv_sem=ag_recv.at[s, c],
            device_id={"mp": me + 2 * up - 1},
            device_id_type=pl.DeviceIdType.MESH,
        )

    def gain_copy(origin, target):
        return pltpu.make_async_remote_copy(
            src_ref=pre,
            dst_ref=gain_all.at[feats_at(origin)],
            send_sem=g_send.at[target],
            recv_sem=g_recv.at[origin],
            device_id={"mp": target},
            device_id_type=pl.DeviceIdType.MESH,
        )

    def w_slot(o):
        return w_all.at[:, pl.ds(pl.multiple_of(o * wrows, wrows), wrows), :]

    def o_slot(o):
        block = pl.ds(pl.multiple_of(o * wcols, wcols), wcols)
        return wo_all.at[:, block] if wide else wo_all.at[block, :]

    def weight_copy(which, o, target, forward):
        slot, ref, send, recv = (
            (w_slot, win, w_send, w_recv) if which == 0 else (o_slot, wout, o_send, o_recv)
        )
        return pltpu.make_async_remote_copy(
            src_ref=slot(o) if forward else ref,
            dst_ref=slot(o),
            send_sem=send.at[1, o] if forward else send.at[0, target],
            recv_sem=recv.at[o],
            device_id={"dp": target},
            device_id_type=pl.DeviceIdType.MESH,
        )

    def rs_copy(s, c, up):
        return pltpu.make_async_remote_copy(
            src_ref=out_buf.at[s, rows_at(c)],
            dst_ref=(from_below if up else from_above).at[s, rows_at(c)],
            send_sem=rs_send.at[s, c],
            recv_sem=rs_recv.at[up, s, c],
            device_id={"mp": me + 2 * up - 1},
            device_id_type=pl.DeviceIdType.MESH,
        )

    def ss_copy(origin, c, target):
        return pltpu.make_async_remote_copy(
            src_ref=ss_mine.at[c],
            dst_ref=ss_all.at[origin, c],
            send_sem=ss_send.at[target, c],
            recv_sem=ss_recv.at[origin, c],
            device_id={"mp": target},
            device_id_type=pl.DeviceIdType.MESH,
        )

    def loop(count, body, start=0):
        def wrapped(i, carry):
            body(i)
            return carry

        lax.fori_loop(start, count, wrapped, 0)

    def local_copies():
        return (
            pltpu.make_async_copy(win, w_slot(d), local_sem.at[0]),
            pltpu.make_async_copy(wout, o_slot(d), local_sem.at[1]),
            pltpu.make_async_copy(tok, x_all.at[me], local_sem.at[2]),
            pltpu.make_async_copy(pre, gain_all.at[feats_at(me)], local_sem.at[3]),
            pltpu.make_async_copy(bias, bias_v, local_sem.at[4]),
        )

    for copy in local_copies():
        copy.start()

    barrier = pltpu.get_barrier_semaphore()

    def greet_mp(k):
        pl.semaphore_signal(
            barrier,
            inc=1,
            device_id={"mp": lax.rem(me + k, n)},
            device_id_type=pl.DeviceIdType.MESH,
        )

    def greet_dp(k):
        pl.semaphore_signal(
            barrier,
            inc=1,
            device_id={"dp": lax.rem(d + k, groups)},
            device_id_type=pl.DeviceIdType.MESH,
        )

    loop(n, greet_mp, 1)
    loop(groups, greet_dp, 1)
    pl.semaphore_wait(barrier, n - 1 + groups - 1)

    def peer_mp(k):
        return lax.rem(me + k, n)

    def same_core(k):
        return 2 * lax.rem(pair + k, half) + odd

    def from_core(k):
        return 2 * lax.rem(pair + half - k, half) + odd

    loop(n, lambda k: gain_copy(me, peer_mp(k)).start(), 1)
    def send_own(up):
        @pl.when((me < n - 1) if up else (me > 0))
        def _():
            @pl.when(odd == 1)
            def _():
                pl.semaphore_wait(link_free.at[up], 1)

            loop(chunks, lambda c: tok_copy(me, c, up, True).start())

    def release(up):
        s = 0 if up else n - 1

        @pl.when(((me < n - 1) if up else (me > 0)) & (odd == 0))
        def _():
            loop(chunks, lambda c: tok_copy(s, c, up, False).wait_send())
            pl.semaphore_signal(
                link_free.at[up],
                inc=1,
                device_id={"dp": partner},
                device_id_type=pl.DeviceIdType.MESH,
            )

    def send_both():
        @pl.when(2 * me < n)
        def _():
            send_own(1)
            send_own(0)

        @pl.when(2 * me >= n)
        def _():
            send_own(0)
            send_own(1)

    pl.when(odd == 0)(send_both)
    weight_copy(0, d, partner, False).start()
    loop(half, lambda k: weight_copy(0, d, same_core(k), False).start(), 1)
    weight_copy(1, d, partner, False).start()
    loop(half, lambda k: weight_copy(1, d, same_core(k), False).start(), 1)

    pl.when((odd == 0) & (me == 0))(lambda: release(1))
    pl.when((odd == 0) & (me == n - 1))(lambda: release(0))

    acc[...] = jnp.zeros_like(acc)
    square[...] = jnp.zeros_like(square)

    def take_shards(j):
        below, above = me - j, me + j

        def one(c):
            @pl.when(below >= 0)
            def _():
                tok_copy(below, c, 1, False).wait_recv()

                @pl.when(me < n - 1)
                def _():
                    tok_copy(below, c, 1, False).start()

            @pl.when(above < n)
            def _():
                tok_copy(above, c, 0, False).wait_recv()

                @pl.when(me > 0)
                def _():
                    tok_copy(above, c, 0, False).start()

        loop(chunks, one)
        pl.when((j == me))(lambda: release(1))
        pl.when((j == n - 1 - me))(lambda: release(0))

    def project(j):
        def side(up):
            s = me + (2 * up - 1) * j

            @pl.when((s >= 0) & (s < n) & ((j > 0) | (up == 0)))
            def _():
                block = feats_at(s)
                gain = gain_all[feats_at(s)].astype(F32).reshape(1, feats)

                x = x_all[s].astype(F32)
                square[...] += x * x
                xg = (x * gain).astype(BF16)
                for m in range(3):
                    acc[m] += jnp.dot(xg, w_all[m, block, :], preferred_element_type=F32)

        loop(2, side)

    def forward_weights(which):
        def forward(k):
            o = from_core(k)
            weight_copy(which, o, partner, False).wait_recv()
            weight_copy(which, o, partner, True).start()

        loop(half, forward, 1)

    def other_weights(which):
        loop(half, lambda k: weight_copy(which, 2 * k + 1 - odd, partner, False).wait_recv())

    @pl.when(odd == 1)
    def _():
        forward_weights(0)
        send_both()
        take_shards(1)
        forward_weights(1)

    @pl.when(odd == 0)
    def _():
        loop(n, take_shards, 1)
        forward_weights(0)

    for copy in local_copies():
        copy.wait()
    loop(n, lambda k: gain_copy(peer_mp(k), peer_mp(k)).wait_recv(), 1)
    other_weights(0)
    loop(2, project)

    def later(j):
        pl.when(odd == 1)(lambda: take_shards(j))
        project(j)

    loop(n, later, 2)
    pl.when(odd == 0)(lambda: forward_weights(1))
    other_weights(1)

    def finish(c):
        total = jnp.sum(square[rows_at(c), :], axis=1, keepdims=True)
        inverse = lax.rsqrt(total / model + epsilon)
        for m in range(3):
            qkv[m, rows_at(c), :] = (acc[m, rows_at(c), :] * inverse).astype(BF16)

    loop(chunks, finish)

    lane_head = lax.broadcasted_iota(jnp.int32, (1, inner), 1) // head_dim
    contract = (((1,), (1,)), ((), ()))

    def send_out(s, c, up, value):
        out_buf[s, rows_at(c), :] = value.astype(BF16)
        rs_copy(s, c, up).start()

    def attend(c):
        first = (c * step) // seq * seq
        keys_at = pl.ds(pl.multiple_of(first, seq), seq)
        bias_at = pl.ds(pl.multiple_of(c * step - first, step), step)
        q = qkv[0, rows_at(c), :]
        k = qkv[1, keys_at, :]
        v = qkv[2, keys_at, :]
        context = jnp.zeros((step, inner), F32)
        for h in range(heads):
            qh = jnp.where(lane_head == h, q, jnp.zeros_like(q))
            scores = lax.dot_general(qh, k, contract, preferred_element_type=F32)
            scores = scores + bias_v[h, bias_at, :].astype(F32)
            weights = jnp.exp(scores - jnp.max(scores, axis=1, keepdims=True))
            scale = 1.0 / jnp.sum(weights, axis=1, keepdims=True)
            mixed = jnp.dot(weights.astype(BF16), v, preferred_element_type=F32)
            context = jnp.where(lane_head == h, mixed * scale, context)
        context = context.astype(BF16)

        def share(s):
            block = feats_at(s)
            if wide:
                value = jnp.dot(context, wo_all[:, block], preferred_element_type=F32)
            else:
                value = lax.dot_general(
                    context, wo_all[block, :], contract, preferred_element_type=F32
                )
            part[s, rows_at(c), :] = value

        for s in range(n):
            share(s)

        @pl.when(me == 0)
        def _():
            loop(n - 1, lambda k: send_out(n - 1 - k, c, 1, part[n - 1 - k, rows_at(c), :]))

        @pl.when(me == n - 1)
        def _():
            loop(n - 1, lambda k: send_out(k, c, 0, part[k, rows_at(c), :]))

    loop(rows // step, attend)

    def finalize(c):
        own = x_all[me, rows_at(c), :].astype(F32) + part[me, rows_at(c), :]
        stream = own.astype(BF16)
        stream_o[rows_at(c), :] = stream
        wide_stream = stream.astype(F32)
        total = jnp.sum(wide_stream * wide_stream, axis=1, keepdims=True)
        turned = jnp.transpose(jnp.broadcast_to(total, (step, 128)))
        ss_mine[c] = turned[0:8, :]
        ss_all[me, c] = turned[0:8, :]
        loop(n, lambda k: ss_copy(me, c, peer_mp(k)).start(), 1)

    messages = chunks * (n - 1)

    def chain(t, up, lead):
        m = t - lead
        landed = from_below if up else from_above

        @pl.when((m >= 0) & (m < messages))
        def _():
            c, k = m // (n - 1), lax.rem(m, n - 1)
            s = n - 1 - k if up else k
            further = s > me if up else s < me

            @pl.when(further | (s == me))
            def _():
                rs_copy(s, c, up).wait_recv()
                value = part[s, rows_at(c), :] + landed[s, rows_at(c), :].astype(F32)

                @pl.when(s == me)
                def _():
                    part[s, rows_at(c), :] = value

                @pl.when(further)
                def _():
                    send_out(s, c, up, value)

    up_lead, down_lead = (me - 1) * lag, (n - 2 - me) * lag
    up_last, down_last = n - 1 - me + up_lead, me + down_lead
    last = jnp.where(
        me == 0, down_last, jnp.where(me == n - 1, up_last, jnp.maximum(up_last, down_last))
    )

    def tick(t):
        @pl.when(me > 0)
        def _():
            chain(t, 1, up_lead)

        @pl.when(me < n - 1)
        def _():
            chain(t, 0, down_lead)

        @pl.when((t >= last) & (lax.rem(t - last + n - 1, n - 1) == 0))
        def _():
            c = (t - last + n - 1) // (n - 1) - 1

            @pl.when(c < chunks)
            def _():
                finalize(c)

    loop(messages + (n - 2) * lag, tick)

    def normalize(c):
        loop(n, lambda k: ss_copy(peer_mp(k), c, peer_mp(k)).wait_recv(), 1)
        total = jnp.zeros((8, step), F32)
        for s in range(n):
            total = total + ss_all[s, c]
        post = jnp.transpose(lax.rsqrt(total / model + epsilon))[:, 0:1]
        stream = stream_o[rows_at(c), :].astype(F32)
        gain = post_g[...].astype(F32).reshape(1, feats)
        normed_o[rows_at(c), :] = (stream * post * gain).astype(BF16)

    loop(chunks, normalize)

    loop(n, lambda k: gain_copy(me, peer_mp(k)).wait_send(), 1)

    def drain_tokens(s):
        def one(c):
            @pl.when((s <= me) & (me < n - 1) & ((s > 0) | (odd == 1)))
            def _():
                tok_copy(s, c, 1, False).wait_send()

            @pl.when((s >= me) & (me > 0) & ((s < n - 1) | (odd == 1)))
            def _():
                tok_copy(s, c, 0, False).wait_send()

            @pl.when(s != me)
            def _():
                rs_copy(s, c, 1).wait_send()
                ss_copy(me, c, s).wait_send()

        loop(chunks, one)

    loop(n, drain_tokens)
    for which in range(2):
        weight_copy(which, d, partner, False).wait_send()

        def drain(k):
            weight_copy(which, d, same_core(k), False).wait_send()
            weight_copy(which, from_core(k), partner, True).wait_send()

        loop(half, drain, 1)


def on_device(n, groups, tokens, pre_gain, input_weight, output_weight, position_bias, post_gain):
    rows, feats = tokens.shape
    chunks, lag = rows // 256, 2
    step = rows // chunks
    inner = input_weight.shape[2]
    model = n * feats
    wide = output_weight.shape[1] % 128 == 0
    if not wide:
        output_weight = output_weight.T
    dma, any_space = pltpu.SemaphoreType.DMA, pl.BlockSpec(memory_space=pl.ANY)
    shape = jax.ShapeDtypeStruct((rows, feats), BF16)
    return pl.pallas_call(
        functools.partial(kernel, n, groups, chunks, lag, wide),
        out_shape=(shape, shape),
        in_specs=[any_space] * 2 + [pl.BlockSpec(memory_space=pltpu.VMEM)] + [any_space] * 3,
        out_specs=[pl.BlockSpec(memory_space=pltpu.VMEM)] * 2,
        scratch_shapes=[
            pltpu.VMEM((n, rows, feats), BF16),
            pltpu.VMEM((n * feats,), BF16),
            pltpu.VMEM((3, model, inner), BF16),
            pltpu.VMEM((inner, model) if wide else (model, inner), BF16),
            pltpu.VMEM(position_bias.shape, BF16),
            pltpu.VMEM((3, rows, inner), F32),
            pltpu.VMEM((rows, feats), F32),
            pltpu.VMEM((3, rows, inner), BF16),
            pltpu.VMEM((n, rows, feats), F32),
            pltpu.VMEM((n, rows, feats), BF16),
            pltpu.VMEM((n, rows, feats), BF16),
            pltpu.VMEM((n, rows, feats), BF16),
            pltpu.VMEM((chunks, 8, step), F32),
            pltpu.VMEM((n, chunks, 8, step), F32),
            dma((2, n, chunks)),
            dma((n, chunks)),
            dma((n,)),
            dma((n,)),
            dma((2, groups)),
            dma((groups,)),
            dma((2, groups)),
            dma((groups,)),
            dma((n, chunks)),
            dma((2, n, chunks)),
            dma((n, chunks)),
            dma((n, chunks)),
            dma((5,)),
            pltpu.SemaphoreType.REGULAR((2,)),
        ],
        compiler_params=pltpu.CompilerParams(
            collective_id=0, has_side_effects=True, vmem_limit_bytes=56 * 1024 * 1024
        ),
    )(tokens, pre_gain, post_gain, input_weight, output_weight, position_bias)


def solution(mesh):
    return jax.shard_map(
        functools.partial(on_device, mesh.shape["mp"], mesh.shape["dp"]),
        mesh=mesh,
        in_specs=(
            P("dp", "mp"),
            P("mp"),
            P(None, "dp", "mp"),
            P("mp", "dp"),
            P("mp", None, None),
            P("mp"),
        ),
        out_specs=(P("dp", "mp"), P("dp", "mp")),
        check_vma=False,
    )
```

```python
import functools

import jax
import jax.numpy as jnp
from jax import lax
from jax.experimental import pallas as pl
from jax.experimental.pallas import tpu as pltpu
from jax.sharding import PartitionSpec as P

epsilon = 1e-06
F32, BF16 = jnp.float32, jnp.bfloat16


def kernel(
    n,
    groups,
    chunks,
    lag,
    wide,
    tok,
    pre,
    win,
    wout,
    bias,
    stream_o,
    square_o,
    x_all,
    gain_all,
    w_all,
    wo_all,
    bias_v,
    acc,
    square,
    qkv,
    part,
    out_buf,
    from_below,
    from_above,
    ss_mine,
    ss_all,
    ag_send,
    ag_recv,
    g_send,
    g_recv,
    w_send,
    w_recv,
    o_send,
    o_recv,
    rs_send,
    rs_recv,
    ss_send,
    ss_recv,
    local_sem,
    link_free,
):
    rows, feats = tok.shape
    step = rows // chunks
    heads, seq = bias.shape[0], bias.shape[1]
    inner = win.shape[2]
    head_dim = inner // heads
    model = n * feats
    wrows = win.shape[1]
    wcols = model // groups
    half = groups // 2
    me = lax.axis_index("mp")
    d = lax.axis_index("dp")
    odd = lax.rem(d, 2)
    pair = d // 2
    partner = d + 1 - 2 * odd

    def rows_at(c):
        return pl.ds(pl.multiple_of(c * step, step), step)

    def feats_at(s):
        return pl.ds(pl.multiple_of(s * feats, feats), feats)

    def tok_copy(s, c, up, own):
        src = tok.at[rows_at(c)] if own else x_all.at[s, rows_at(c)]
        return pltpu.make_async_remote_copy(
            src_ref=src,
            dst_ref=x_all.at[s, rows_at(c)],
            send_sem=ag_send.at[up, s, c],
            recv_sem=ag_recv.at[s, c],
            device_id={"mp": me + 2 * up - 1},
            device_id_type=pl.DeviceIdType.MESH,
        )

    def gain_copy(origin, target):
        return pltpu.make_async_remote_copy(
            src_ref=pre,
            dst_ref=gain_all.at[feats_at(origin)],
            send_sem=g_send.at[target],
            recv_sem=g_recv.at[origin],
            device_id={"mp": target},
            device_id_type=pl.DeviceIdType.MESH,
        )

    def w_slot(o):
        return w_all.at[:, pl.ds(pl.multiple_of(o * wrows, wrows), wrows), :]

    def o_slot(o):
        block = pl.ds(pl.multiple_of(o * wcols, wcols), wcols)
        return wo_all.at[:, block] if wide else wo_all.at[block, :]

    def weight_copy(which, o, target, forward):
        slot, ref, send, recv = (
            (w_slot, win, w_send, w_recv) if which == 0 else (o_slot, wout, o_send, o_recv)
        )
        return pltpu.make_async_remote_copy(
            src_ref=slot(o) if forward else ref,
            dst_ref=slot(o),
            send_sem=send.at[1, o] if forward else send.at[0, target],
            recv_sem=recv.at[o],
            device_id={"dp": target},
            device_id_type=pl.DeviceIdType.MESH,
        )

    def rs_copy(s, c, up):
        return pltpu.make_async_remote_copy(
            src_ref=out_buf.at[s, rows_at(c)],
            dst_ref=(from_below if up else from_above).at[s, rows_at(c)],
            send_sem=rs_send.at[s, c],
            recv_sem=rs_recv.at[up, s, c],
            device_id={"mp": me + 2 * up - 1},
            device_id_type=pl.DeviceIdType.MESH,
        )

    def ss_copy(origin, c, target):
        return pltpu.make_async_remote_copy(
            src_ref=ss_mine.at[c],
            dst_ref=ss_all.at[origin, c],
            send_sem=ss_send.at[target, c],
            recv_sem=ss_recv.at[origin, c],
            device_id={"mp": target},
            device_id_type=pl.DeviceIdType.MESH,
        )

    def loop(count, body, start=0):
        def wrapped(i, carry):
            body(i)
            return carry

        lax.fori_loop(start, count, wrapped, 0)

    def local_copies():
        return (
            pltpu.make_async_copy(win, w_slot(d), local_sem.at[0]),
            pltpu.make_async_copy(wout, o_slot(d), local_sem.at[1]),
            pltpu.make_async_copy(tok, x_all.at[me], local_sem.at[2]),
            pltpu.make_async_copy(pre, gain_all.at[feats_at(me)], local_sem.at[3]),
            pltpu.make_async_copy(bias, bias_v, local_sem.at[4]),
        )

    for copy in local_copies():
        copy.start()

    barrier = pltpu.get_barrier_semaphore()

    def greet_mp(k):
        pl.semaphore_signal(
            barrier,
            inc=1,
            device_id={"mp": lax.rem(me + k, n)},
            device_id_type=pl.DeviceIdType.MESH,
        )

    def greet_dp(k):
        pl.semaphore_signal(
            barrier,
            inc=1,
            device_id={"dp": lax.rem(d + k, groups)},
            device_id_type=pl.DeviceIdType.MESH,
        )

    loop(n, greet_mp, 1)
    loop(groups, greet_dp, 1)
    pl.semaphore_wait(barrier, n - 1 + groups - 1)

    def peer_mp(k):
        return lax.rem(me + k, n)

    def same_core(k):
        return 2 * lax.rem(pair + k, half) + odd

    def from_core(k):
        return 2 * lax.rem(pair + half - k, half) + odd

    loop(n, lambda k: gain_copy(me, peer_mp(k)).start(), 1)
    def send_own(up):
        @pl.when((me < n - 1) if up else (me > 0))
        def _():
            @pl.when(odd == 1)
            def _():
                pl.semaphore_wait(link_free.at[up], 1)

            loop(chunks, lambda c: tok_copy(me, c, up, True).start())

    def release(up):
        s = 0 if up else n - 1

        @pl.when(((me < n - 1) if up else (me > 0)) & (odd == 0))
        def _():
            loop(chunks, lambda c: tok_copy(s, c, up, False).wait_send())
            pl.semaphore_signal(
                link_free.at[up],
                inc=1,
                device_id={"dp": partner},
                device_id_type=pl.DeviceIdType.MESH,
            )

    def send_both():
        @pl.when(2 * me < n)
        def _():
            send_own(1)
            send_own(0)

        @pl.when(2 * me >= n)
        def _():
            send_own(0)
            send_own(1)

    pl.when(odd == 0)(send_both)
    weight_copy(0, d, partner, False).start()
    loop(half, lambda k: weight_copy(0, d, same_core(k), False).start(), 1)
    weight_copy(1, d, partner, False).start()
    loop(half, lambda k: weight_copy(1, d, same_core(k), False).start(), 1)

    pl.when((odd == 0) & (me == 0))(lambda: release(1))
    pl.when((odd == 0) & (me == n - 1))(lambda: release(0))

    acc[...] = jnp.zeros_like(acc)
    square[...] = jnp.zeros_like(square)

    def take_shards(j):
        below, above = me - j, me + j

        def one(c):
            @pl.when(below >= 0)
            def _():
                tok_copy(below, c, 1, False).wait_recv()

                @pl.when(me < n - 1)
                def _():
                    tok_copy(below, c, 1, False).start()

            @pl.when(above < n)
            def _():
                tok_copy(above, c, 0, False).wait_recv()

                @pl.when(me > 0)
                def _():
                    tok_copy(above, c, 0, False).start()

        loop(chunks, one)
        pl.when((j == me))(lambda: release(1))
        pl.when((j == n - 1 - me))(lambda: release(0))

    def project(j):
        def side(up):
            s = me + (2 * up - 1) * j

            @pl.when((s >= 0) & (s < n) & ((j > 0) | (up == 0)))
            def _():
                block = feats_at(s)
                gain = gain_all[feats_at(s)].astype(F32).reshape(1, feats)

                x = x_all[s].astype(F32)
                square[...] += x * x
                xg = (x * gain).astype(BF16)
                for m in range(3):
                    acc[m] += jnp.dot(xg, w_all[m, block, :], preferred_element_type=F32)

        loop(2, side)

    def forward_weights(which):
        def forward(k):
            o = from_core(k)
            weight_copy(which, o, partner, False).wait_recv()
            weight_copy(which, o, partner, True).start()

        loop(half, forward, 1)

    def other_weights(which):
        loop(half, lambda k: weight_copy(which, 2 * k + 1 - odd, partner, False).wait_recv())

    @pl.when(odd == 1)
    def _():
        forward_weights(0)
        send_both()
        take_shards(1)
        forward_weights(1)

    @pl.when(odd == 0)
    def _():
        loop(n, take_shards, 1)
        forward_weights(0)

    for copy in local_copies():
        copy.wait()
    loop(n, lambda k: gain_copy(peer_mp(k), peer_mp(k)).wait_recv(), 1)
    other_weights(0)
    loop(2, project)

    def later(j):
        pl.when(odd == 1)(lambda: take_shards(j))
        project(j)

    loop(n, later, 2)
    pl.when(odd == 0)(lambda: forward_weights(1))
    other_weights(1)

    def finish(c):
        total = jnp.sum(square[rows_at(c), :], axis=1, keepdims=True)
        inverse = lax.rsqrt(total / model + epsilon)
        for m in range(3):
            qkv[m, rows_at(c), :] = (acc[m, rows_at(c), :] * inverse).astype(BF16)

    loop(chunks, finish)

    lane_head = lax.broadcasted_iota(jnp.int32, (1, inner), 1) // head_dim
    contract = (((1,), (1,)), ((), ()))

    def send_out(s, c, up, value):
        out_buf[s, rows_at(c), :] = value.astype(BF16)
        rs_copy(s, c, up).start()

    def attend(c):
        first = (c * step) // seq * seq
        keys_at = pl.ds(pl.multiple_of(first, seq), seq)
        bias_at = pl.ds(pl.multiple_of(c * step - first, step), step)
        q = qkv[0, rows_at(c), :]
        k = qkv[1, keys_at, :]
        v = qkv[2, keys_at, :]
        context = jnp.zeros((step, inner), F32)
        for h in range(heads):
            qh = jnp.where(lane_head == h, q, jnp.zeros_like(q))
            scores = lax.dot_general(qh, k, contract, preferred_element_type=F32)
            scores = scores + bias_v[h, bias_at, :].astype(F32)
            weights = jnp.exp(scores - jnp.max(scores, axis=1, keepdims=True))
            scale = 1.0 / jnp.sum(weights, axis=1, keepdims=True)
            mixed = jnp.dot(weights.astype(BF16), v, preferred_element_type=F32)
            context = jnp.where(lane_head == h, mixed * scale, context)
        context = context.astype(BF16)

        def share(s):
            block = feats_at(s)
            if wide:
                value = jnp.dot(context, wo_all[:, block], preferred_element_type=F32)
            else:
                value = lax.dot_general(
                    context, wo_all[block, :], contract, preferred_element_type=F32
                )
            part[s, rows_at(c), :] = value

        for s in range(n):
            share(s)

        @pl.when(me == 0)
        def _():
            loop(n - 1, lambda k: send_out(n - 1 - k, c, 1, part[n - 1 - k, rows_at(c), :]))

        @pl.when(me == n - 1)
        def _():
            loop(n - 1, lambda k: send_out(k, c, 0, part[k, rows_at(c), :]))

    loop(rows // step, attend)

    def finalize(c):
        own = x_all[me, rows_at(c), :].astype(F32) + part[me, rows_at(c), :]
        stream = own.astype(BF16)
        stream_o[rows_at(c), :] = stream
        wide_stream = stream.astype(F32)
        total = jnp.sum(wide_stream * wide_stream, axis=1, keepdims=True)
        turned = jnp.transpose(jnp.broadcast_to(total, (step, 128)))
        ss_mine[c] = turned[0:8, :]
        ss_all[me, c] = turned[0:8, :]
        loop(n, lambda k: ss_copy(me, c, peer_mp(k)).start(), 1)

    messages = chunks * (n - 1)

    def chain(t, up, lead):
        m = t - lead
        landed = from_below if up else from_above

        @pl.when((m >= 0) & (m < messages))
        def _():
            c, k = m // (n - 1), lax.rem(m, n - 1)
            s = n - 1 - k if up else k
            further = s > me if up else s < me

            @pl.when(further | (s == me))
            def _():
                rs_copy(s, c, up).wait_recv()
                value = part[s, rows_at(c), :] + landed[s, rows_at(c), :].astype(F32)

                @pl.when(s == me)
                def _():
                    part[s, rows_at(c), :] = value

                @pl.when(further)
                def _():
                    send_out(s, c, up, value)

    up_lead, down_lead = (me - 1) * lag, (n - 2 - me) * lag
    up_last, down_last = n - 1 - me + up_lead, me + down_lead
    last = jnp.where(
        me == 0, down_last, jnp.where(me == n - 1, up_last, jnp.maximum(up_last, down_last))
    )

    def tick(t):
        @pl.when(me > 0)
        def _():
            chain(t, 1, up_lead)

        @pl.when(me < n - 1)
        def _():
            chain(t, 0, down_lead)

        @pl.when((t >= last) & (lax.rem(t - last + n - 1, n - 1) == 0))
        def _():
            c = (t - last + n - 1) // (n - 1) - 1

            @pl.when(c < chunks)
            def _():
                finalize(c)

    loop(messages + (n - 2) * lag, tick)

    def normalize(c):
        loop(n, lambda k: ss_copy(peer_mp(k), c, peer_mp(k)).wait_recv(), 1)
        total = jnp.zeros((8, step), F32)
        for s in range(n):
            total = total + ss_all[s, c]
        square_o[c] = total

    loop(chunks, normalize)

    loop(n, lambda k: gain_copy(me, peer_mp(k)).wait_send(), 1)

    def drain_tokens(s):
        def one(c):
            @pl.when((s <= me) & (me < n - 1) & ((s > 0) | (odd == 1)))
            def _():
                tok_copy(s, c, 1, False).wait_send()

            @pl.when((s >= me) & (me > 0) & ((s < n - 1) | (odd == 1)))
            def _():
                tok_copy(s, c, 0, False).wait_send()

            @pl.when(s != me)
            def _():
                rs_copy(s, c, 1).wait_send()
                ss_copy(me, c, s).wait_send()

        loop(chunks, one)

    loop(n, drain_tokens)
    for which in range(2):
        weight_copy(which, d, partner, False).wait_send()

        def drain(k):
            weight_copy(which, d, same_core(k), False).wait_send()
            weight_copy(which, from_core(k), partner, True).wait_send()

        loop(half, drain, 1)


def post_norm(model, stream_i, square_i, gain_i, stream_o, normed_o):
    chunks, _, step = square_i.shape
    gain = gain_i[...].astype(F32).reshape(1, stream_i.shape[1])
    for c in range(chunks):
        post = jnp.transpose(lax.rsqrt(square_i[c] / model + epsilon))[:, 0:1]
        stream = stream_i[c * step : (c + 1) * step, :]
        stream_o[c * step : (c + 1) * step, :] = stream
        normed_o[c * step : (c + 1) * step, :] = (stream.astype(F32) * post * gain).astype(BF16)


def on_device(n, groups, tokens, pre_gain, input_weight, output_weight, position_bias, post_gain):
    rows, feats = tokens.shape
    chunks, lag = rows // 256, 2
    step = rows // chunks
    inner = input_weight.shape[2]
    model = n * feats
    wide = output_weight.shape[1] % 128 == 0
    if not wide:
        output_weight = output_weight.T
    dma, any_space = pltpu.SemaphoreType.DMA, pl.BlockSpec(memory_space=pl.ANY)
    shape = jax.ShapeDtypeStruct((rows, feats), BF16)
    stream, squares = pl.pallas_call(
        functools.partial(kernel, n, groups, chunks, lag, wide),
        out_shape=(shape, jax.ShapeDtypeStruct((chunks, 8, step), F32)),
        in_specs=[any_space] * 5,
        out_specs=[pl.BlockSpec(memory_space=pltpu.VMEM)] * 2,
        scratch_shapes=[
            pltpu.VMEM((n, rows, feats), BF16),
            pltpu.VMEM((n * feats,), BF16),
            pltpu.VMEM((3, model, inner), BF16),
            pltpu.VMEM((inner, model) if wide else (model, inner), BF16),
            pltpu.VMEM(position_bias.shape, BF16),
            pltpu.VMEM((3, rows, inner), F32),
            pltpu.VMEM((rows, feats), F32),
            pltpu.VMEM((3, rows, inner), BF16),
            pltpu.VMEM((n, rows, feats), F32),
            pltpu.VMEM((n, rows, feats), BF16),
            pltpu.VMEM((n, rows, feats), BF16),
            pltpu.VMEM((n, rows, feats), BF16),
            pltpu.VMEM((chunks, 8, step), F32),
            pltpu.VMEM((n, chunks, 8, step), F32),
            dma((2, n, chunks)),
            dma((n, chunks)),
            dma((n,)),
            dma((n,)),
            dma((2, groups)),
            dma((groups,)),
            dma((2, groups)),
            dma((groups,)),
            dma((n, chunks)),
            dma((2, n, chunks)),
            dma((n, chunks)),
            dma((n, chunks)),
            dma((5,)),
            pltpu.SemaphoreType.REGULAR((2,)),
        ],
        compiler_params=pltpu.CompilerParams(
            collective_id=0, has_side_effects=True, vmem_limit_bytes=56 * 1024 * 1024
        ),
    )(tokens, pre_gain, input_weight, output_weight, position_bias)
    vmem = pl.BlockSpec(memory_space=pltpu.VMEM)
    return pl.pallas_call(
        functools.partial(post_norm, model),
        out_shape=(shape, shape),
        in_specs=[vmem] * 3,
        out_specs=[vmem] * 2,
        compiler_params=pltpu.CompilerParams(vmem_limit_bytes=8 * 1024 * 1024),
    )(stream, squares, post_gain)


def solution(mesh):
    return jax.shard_map(
        functools.partial(on_device, mesh.shape["mp"], mesh.shape["dp"]),
        mesh=mesh,
        in_specs=(
            P("dp", "mp"),
            P("mp"),
            P(None, "dp", "mp"),
            P("mp", "dp"),
            P("mp", None, None),
            P("mp"),
        ),
        out_specs=(P("dp", "mp"), P("dp", "mp")),
        check_vma=False,
    )
```
